256 devices in a mesh: dp: 32 (over y, z), mp: 8 (over x, core).
Axes of the slice: x: 4, y: 4, z: 8, core: 2. Of those that a mesh axis runs over, the one named last changes fastest.
Arguments:
- grad_parts: bfloat16 [32, 8, 1024, 1024], P('dp', 'mp'), may hold values from -10 to 10
- left_stat: float32 [8, 1024, 1024], P('mp', 'dp'), may hold values from -60 to 500, as said below
- right_stat: float32 [8, 1024, 1024], P('mp', 'dp'), may hold values from -60 to 500, as said below
- left_root: bfloat16 [8, 1024, 1024], P('mp', 'dp'), may hold values from -2 to 2
- right_root: bfloat16 [8, 1024, 1024], P('mp', 'dp'), may hold values from -2 to 2
- due: int32 [8, 2], P('mp'), may hold values 0 or 1
Outputs:
- update: bfloat16 [8, 1024, 1024], P('mp')
- left_new: float32 [8, 1024, 1024], P('mp', 'dp')
- right_new: float32 [8, 1024, 1024], P('mp', 'dp')
- left_out: bfloat16 [8, 1024, 1024], P('mp', 'dp')
- right_out: bfloat16 [8, 1024, 1024], P('mp', 'dp')
The draws below stay inside these ranges and needn't reach their ends.
Inputs may be any that keep to these rules, and one draw needn't show every extreme that they name: `left_stat`: every block is positive definite. `right_stat`: every block is positive definite. `due`: 1 where that statistic of the block gets a new root in this step.
All inputs are finite; a program needn't handle non-finite values.
Results may differ from the reference program's by a relative error of at most 0.022.
Values may be sent and summed in bfloat16 or wider, within the bound.
No kernel may reach another device: no remote copies, remote signals or barrier semaphores. Data moves between devices by JAX's collectives and lax.ppermute only.
A program may use at most 64 MiB of HBM per device.

```python
import math
import jax
import jax.numpy as jnp
from jax import lax

B = 1024
BLOCKS = 8
PARTIALS = 32


def draw_grad_parts(key, part):
    base = jnp.clip(jax.random.normal(key, (PARTIALS, BLOCKS, B, B), jnp.float32), -5.0, 5.0)
    ramp = 0.6 + 1.2 * jnp.arange(B, dtype=jnp.float32) / B
    values = 0.4 * base * ramp[None, None, :, None]
    return jnp.clip(values, -10.0, 10.0).astype(jnp.bfloat16)


def make_statistic(key, salt):
    inner = jax.random.fold_in(key, salt)
    matrices = jax.random.normal(jax.random.fold_in(inner, 1), (BLOCKS, B, B), jnp.float32)
    gram = jnp.einsum('bij,bkj->bik', matrices, matrices, precision=lax.Precision.HIGHEST) / B
    ramp = 0.25 + 2.75 * jnp.arange(B, dtype=jnp.float32) / B
    statistic = gram + (jnp.eye(B, dtype=jnp.float32) * ramp[None, :])[None]
    return statistic


def make_root(key, salt):
    inner = jax.random.fold_in(key, salt)
    noise = jnp.clip(jax.random.normal(jax.random.fold_in(inner, 1), (BLOCKS, B, B), jnp.float32), -5.0, 5.0)
    diagonal = jax.random.uniform(jax.random.fold_in(inner, 2), (BLOCKS, B), jnp.float32, 0.5, 0.9)
    spread = 0.35
    values = spread * noise / math.sqrt(B) + jnp.eye(B, dtype=jnp.float32)[None] * diagonal[:, :, None]
    return values.astype(jnp.bfloat16)


def draw_left_stat(key, part):
    return make_statistic(key, 101)


def draw_right_stat(key, part):
    return make_statistic(key, 202)


def draw_left_root(key, part):
    return make_root(key, 303)


def draw_right_root(key, part):
    return make_root(key, 404)


def with_ends(values, rng, low, high):
    longest = values.shape.index(max(values.shape))
    spots = []
    for shift in (0, 1):
        where = [jax.random.randint(jax.random.fold_in(rng, axis), (), 0, length) for axis, length in enumerate(values.shape)]
        where[longest] = (where[longest] + shift) % values.shape[longest]
        spots.append(tuple(where))
    return values.at[spots[0]].set(low).at[spots[1]].set(high)


def setup_inputs(seed: int = 0) -> dict:
    streams_of = jax.random.split(jax.random.key(seed), 7)
    grad_parts = draw_grad_parts(jax.random.fold_in(streams_of[6], 71), 0)
    left_stat = draw_left_stat(jax.random.fold_in(streams_of[6], 71), 0)
    right_stat = draw_right_stat(jax.random.fold_in(streams_of[6], 71), 0)
    left_root = draw_left_root(jax.random.fold_in(streams_of[6], 71), 0)
    right_root = draw_right_root(jax.random.fold_in(streams_of[6], 71), 0)
    due = with_ends((jax.random.randint(streams_of[5], (BLOCKS, 2), 0, 2) < 1).astype(jnp.int32), jax.random.fold_in(streams_of[5], 1), 0, 1)
    return {"grad_parts": grad_parts, "left_stat": left_stat, "right_stat": right_stat, "left_root": left_root, "right_root": right_root, "due": due}


epsilon = 1e-06
decay = 0.9

def root_inverse(statistic):
    order_size = statistic.shape[0]
    scale_c = 4.0 * jnp.trace(statistic) / order_size
    identity = jnp.eye(order_size, dtype=jnp.float32)
    initial = ((5.0 * identity - statistic / scale_c) / 4.0).astype(jnp.bfloat16)
    square = jnp.dot(initial, initial, preferred_element_type=jnp.float32).astype(jnp.bfloat16)
    fourth = jnp.dot(square, square, preferred_element_type=jnp.float32).astype(jnp.bfloat16)
    combined = (5.0 * initial.astype(jnp.float32) - 4.0 * square.astype(jnp.float32)).astype(jnp.bfloat16)
    product = jnp.dot(fourth, combined, preferred_element_type=jnp.float32)
    return (scale_c ** (-0.25) * (5.0 * initial.astype(jnp.float32) - product) / 4.0).astype(jnp.bfloat16)

def reference(grad_parts, left_stat, right_stat, left_root, right_root, due):
    gradient = lax.optimization_barrier(jnp.sum(grad_parts, axis=0, dtype=jnp.float32)).astype(jnp.bfloat16)
    squares = jnp.sum(gradient.astype(jnp.float32) ** 2)
    entry_count = gradient.shape[0] * gradient.shape[1] * gradient.shape[2]
    factor = 1.0 / jnp.sqrt(squares / entry_count + epsilon)

    def one_block(items):
        grad_block, left_old, right_old, left_prev, right_prev, flags = items
        order_size = grad_block.shape[0]
        left_prod = jnp.dot(grad_block, grad_block.T, preferred_element_type=jnp.float32)
        right_prod = jnp.dot(grad_block.T, grad_block, preferred_element_type=jnp.float32)
        left_next = left_old * decay + left_prod * ((1.0 - decay) / order_size)
        right_next = right_old * decay + right_prod * ((1.0 - decay) / order_size)
        left_use = jnp.where(flags[0] == 1, root_inverse(left_next), left_prev)
        right_use = jnp.where(flags[1] == 1, root_inverse(right_next), right_prev)
        x_block = jnp.dot(left_use, grad_block, preferred_element_type=jnp.float32).astype(jnp.bfloat16)
        result = jnp.dot(x_block, right_use, preferred_element_type=jnp.float32)
        return (left_next, right_next, left_use, right_use, (result * factor).astype(jnp.bfloat16))
    left_new, right_new, left_out, right_out, update = lax.map(one_block, (gradient, left_stat, right_stat, left_root, right_root, due))
    return (update, left_new, right_new, left_out, right_out)
```

```python
import jax
import jax.numpy as jnp
from jax import lax
from jax.sharding import Mesh
from jax.sharding import PartitionSpec as P

DP = ("y", "zh", "zl")
MP = ("x", "c")
WIDE = ("y", "zl")
NARROW = "zh"

epsilon = 1e-06
decay = 0.9


def dot(a, b, dims):
    return lax.dot_general(a, b, (dims, ((), ())), preferred_element_type=jnp.float32)


def exchange_sum(value, axes):
    groups = lax.axis_size(axes)
    parts = value.reshape(groups, value.shape[0] // groups, value.shape[1])
    parts = lax.all_to_all(parts, axes, 0, 0, tiled=True)
    return jnp.sum(parts.astype(jnp.float32), 0).astype(jnp.bfloat16)


def spread(value, axes):
    groups = lax.axis_size(axes)
    copies = jnp.broadcast_to(value[None], (groups, *value.shape))
    parts = lax.all_to_all(copies, axes, 0, 0, tiled=True)
    return parts.reshape(groups * value.shape[0], value.shape[1])


def sum_over_blocks(value):
    for axis in MP:
        size = lax.axis_size(axis)
        step = 1
        while step < size:
            pairs = [(i, i ^ step) for i in range(size)]
            value = value + lax.ppermute(value, axis, pairs)
            step *= 2
    return value


def used_root(product, selected, trace, due):
    order_size = product.shape[0]
    scale_c = 4.0 * trace / order_size
    statistic = decay * selected.astype(jnp.float32) + ((1.0 - decay) / order_size) * product
    identity = jnp.eye(order_size, dtype=jnp.float32)
    initial = ((5.0 * identity - statistic / scale_c) / 4.0).astype(jnp.bfloat16)
    last_first = ((1,), (0,))
    square = dot(initial, initial, last_first).astype(jnp.bfloat16)
    fourth = dot(square, square, last_first).astype(jnp.bfloat16)
    combined = (5.0 * initial.astype(jnp.float32) - 4.0 * square.astype(jnp.float32)).astype(
        jnp.bfloat16
    )
    inner = dot(fourth, combined, last_first)
    root = (scale_c ** (-0.25) * (5.0 * initial.astype(jnp.float32) - inner) / 4.0).astype(
        jnp.bfloat16
    )
    return jnp.where(due == 1, root, selected)


def per_device(grad_parts, left_stat, right_stat, left_root, right_root, due):
    due_left, due_right = due[0, 0], due[0, 1]
    order_size = grad_parts.shape[-1]
    row_count = left_stat.shape[1]
    row_start = lax.axis_index(DP) * row_count
    chosen = jnp.stack(
        [
            jnp.where(due_left == 1, left_stat[0].astype(jnp.bfloat16), left_root[0]),
            jnp.where(due_right == 1, right_stat[0].astype(jnp.bfloat16), right_root[0]),
        ]
    )
    chosen = lax.all_gather(chosen, DP, axis=1, tiled=True)

    rows = exchange_sum(exchange_sum(grad_parts[0, 0], WIDE), NARROW)
    grad = spread(spread(rows, NARROW), WIDE)

    squares = jnp.sum(grad.astype(jnp.float32) ** 2)
    total = sum_over_blocks(jnp.full((8, 128), squares, jnp.float32))[0, 0]
    entry_count = float(lax.axis_size(MP) * order_size * order_size)
    factor = 1.0 / jnp.sqrt(total / entry_count + epsilon)

    own_rows = lax.dynamic_slice_in_dim(grad, row_start, row_count, 0)
    own_cols = lax.dynamic_slice_in_dim(grad, row_start, row_count, 1)
    weight = (1.0 - decay) / order_size
    left_new = left_stat[0] * decay + dot(own_rows, grad, ((1,), (1,))) * weight
    right_new = right_stat[0] * decay + dot(own_cols, grad, ((0,), (0,))) * weight

    left_all, right_all = chosen[0], chosen[1]
    left_trace = decay * jnp.trace(left_all.astype(jnp.float32)) + weight * squares
    right_trace = decay * jnp.trace(right_all.astype(jnp.float32)) + weight * squares
    left_use = used_root(dot(grad, grad, ((1,), (1,))), left_all, left_trace, due_left)
    right_use = used_root(dot(grad, grad, ((0,), (0,))), right_all, right_trace, due_right)
    x = dot(left_use, grad, ((1,), (0,))).astype(jnp.bfloat16)
    update = (dot(x, right_use, ((1,), (0,))) * factor).astype(jnp.bfloat16)
    left_out = lax.dynamic_slice_in_dim(left_use, row_start, row_count, 0)
    right_out = lax.dynamic_slice_in_dim(right_use, row_start, row_count, 0)
    return (update[None], left_new[None], right_new[None], left_out[None], right_out[None])


def solution(mesh):
    torus = Mesh(mesh.devices.reshape(4, 4, 2, 4, 2), ("y", "zh", "zl", "x", "c"))
    in_specs = (
        P(DP, MP, None, None),
        P(MP, DP, None),
        P(MP, DP, None),
        P(MP, DP, None),
        P(MP, DP, None),
        P(MP, None),
    )
    out_specs = (
        P(MP, None, None),
        P(MP, DP, None),
        P(MP, DP, None),
        P(MP, DP, None),
        P(MP, DP, None),
    )
    return jax.shard_map(
        per_device, mesh=torus, in_specs=in_specs, out_specs=out_specs, check_vma=False
    )
```

```python
import functools

import jax
import jax.numpy as jnp
from jax import lax
from jax.experimental import pallas as pl
from jax.experimental.pallas import tpu as pltpu
from jax.sharding import Mesh
from jax.sharding import PartitionSpec as P

DP = ("y", "zh", "zl")
MP = ("x", "c")
WIDE = ("y", "zl")
NARROW = "zh"

epsilon = 1e-06
decay = 0.9


def dot(a, b, dims):
    return lax.dot_general(a, b, (dims, ((), ())), preferred_element_type=jnp.float32)


def exchange_sum(value, axes):
    groups = lax.axis_size(axes)
    parts = value.reshape(groups, value.shape[0] // groups, value.shape[1])
    parts = lax.all_to_all(parts, axes, 0, 0, tiled=True)
    return jnp.sum(parts.astype(jnp.float32), 0).astype(jnp.bfloat16)


def spread(value, axes):
    groups = lax.axis_size(axes)
    copies = jnp.broadcast_to(value[None], (groups, *value.shape))
    parts = lax.all_to_all(copies, axes, 0, 0, tiled=True)
    return parts.reshape(groups * value.shape[0], value.shape[1])


def choose_kernel(due, left_stat, right_stat, left_root, right_root, chosen):
    for k, stat, root in ((0, left_stat, left_root), (1, right_stat, right_root)):
        chosen[k] = jnp.where(due[0, k] == 1, stat[...].astype(jnp.bfloat16), root[...])


def choose(due, left_stat, right_stat, left_root, right_root):
    vector = pl.BlockSpec(memory_space=pltpu.VMEM)
    return pl.pallas_call(
        choose_kernel,
        out_shape=jax.ShapeDtypeStruct((2, *left_root.shape), jnp.bfloat16),
        in_specs=[pl.BlockSpec(memory_space=pltpu.SMEM), vector, vector, vector, vector],
        out_specs=vector,
        compiler_params=pltpu.CompilerParams(vmem_limit_bytes=4 * 2**20),
        name="choose",
    )(due, left_stat, right_stat, left_root, right_root)


def roots_kernel(tile, *refs):
    mean, due, place, grad, chosen, left_stat, right_stat = refs[:7]
    update, left_new, right_new, left_out, right_out = refs[7:12]
    picked, flipped, first, second, mixed, used, x, fourth, block, sems, sent = refs[12:]
    order = grad.shape[0]
    rows = left_stat.shape[0]
    weight = (1.0 - decay) / order
    columns = [slice(n * tile, (n + 1) * tile) for n in range(order // tile)]
    fetches = [
        pltpu.make_async_copy(chosen.at[k], picked.at[k], sems.at[k]) for k in range(2)
    ]
    for fetch in fetches:
        fetch.start()
    mine = pl.ds(pl.multiple_of(place[0], rows), rows)
    across = ((1,), (0,))
    factor = lax.rsqrt(jnp.full((1, 128), mean[0, 0] + epsilon, jnp.float32))
    factor = jnp.broadcast_to(factor[:, :1], (1, tile))

    def energy():
        total = jnp.zeros((128, order), jnp.float32)
        for i in range(0, order, 128):
            part = grad[i : i + 128, :].astype(jnp.float32)
            total = total + part * part
        return jnp.sum(total)

    squares = energy()

    def scale_of(k):
        row = lax.broadcasted_iota(jnp.int32, (128, 128), 0)
        col = lax.broadcasted_iota(jnp.int32, (128, 128), 1)
        diagonal = jnp.zeros((128, 128), jnp.float32)
        for i in range(0, order, 128):
            part = picked[k, i : i + 128, i : i + 128].astype(jnp.float32)
            diagonal = diagonal + jnp.where(row == col, part, 0.0)
        return (4.0 / order) * (decay * jnp.sum(diagonal) + weight * squares)

    def root_of(k, stat, new, out):
        scale_c = jnp.zeros((1, 128), jnp.float32)
        shrink = lift = None
        for n, cols in enumerate(columns):
            if k == 0:
                product = dot(grad[...], grad[cols, :], ((1,), (1,)))
            else:
                product = dot(flipped[...], grad[:, cols], across)
            if n == 0:
                fetches[k].wait()
                scale_c = scale_c + scale_of(k)
                shrink = jnp.broadcast_to((0.25 / scale_c)[:, :1], (1, tile))
                lift = 0.25 * jnp.exp(-0.25 * jnp.log(scale_c))
                lift = jnp.broadcast_to(lift[:, :1], (1, tile))
            block[:, cols] = product
            row = lax.broadcasted_iota(jnp.int32, (order, tile), 0)
            col = n * tile + lax.broadcasted_iota(jnp.int32, (order, tile), 1)
            statistic = decay * picked[k, :, cols].astype(jnp.float32) + weight * product
            first[:, cols] = (jnp.where(row == col, 1.25, 0.0) - statistic * shrink).astype(
                jnp.bfloat16
            )
        new[...] = stat[...] * decay + block[mine, :] * weight
        for cols in columns:
            square = dot(first[...], first[:, cols], across).astype(jnp.bfloat16)
            second[:, cols] = square
            mixed[:, cols] = (
                5.0 * first[:, cols].astype(jnp.float32) - 4.0 * square.astype(jnp.float32)
            ).astype(jnp.bfloat16)
            if k == 0:
                flipped[cols, :] = grad[:, cols].T
        for cols in columns:
            fourth[:, cols] = dot(second[...], second[:, cols], across).astype(jnp.bfloat16)
        for cols in columns:
            inner = dot(fourth[...], mixed[:, cols], across)
            root = lift * (5.0 * first[:, cols].astype(jnp.float32) - inner)
            used[:, cols] = jnp.where(
                due[0, k] == 1, root.astype(jnp.bfloat16), picked[k, :, cols]
            )
        out[...] = used[mine, :]

    root_of(0, left_stat, left_new, left_out)
    for cols in columns:
        x[:, cols] = dot(used[...], grad[:, cols], across).astype(jnp.bfloat16)
    root_of(1, right_stat, right_new, right_out)
    sends = []
    for n, cols in enumerate(columns):
        fourth[:, cols] = (dot(x[...], used[:, cols], across) * factor).astype(jnp.bfloat16)
        sends.append(
            pltpu.make_async_copy(fourth.at[:, cols], update.at[0, :, cols], sent.at[n])
        )
        sends[-1].start()
    for send in sends:
        send.wait()


def roots(mean, due, place, grad, chosen, left_stat, right_stat):
    order = grad.shape[0]
    tile = 512
    new = jax.ShapeDtypeStruct(left_stat.shape, jnp.float32)
    out = jax.ShapeDtypeStruct(left_stat.shape, jnp.bfloat16)
    scalar = pl.BlockSpec(memory_space=pltpu.SMEM)
    vector = pl.BlockSpec(memory_space=pltpu.VMEM)
    far = pl.BlockSpec(memory_space=pltpu.HBM)
    square = pltpu.VMEM((order, order), jnp.bfloat16)
    return pl.pallas_call(
        functools.partial(roots_kernel, tile),
        out_shape=(jax.ShapeDtypeStruct((1, order, order), jnp.bfloat16), new, new, out, out),
        in_specs=[scalar, scalar, scalar, vector, far, vector, vector],
        out_specs=(far, vector, vector, vector, vector),
        scratch_shapes=[
            pltpu.VMEM((2, order, order), jnp.bfloat16),
            *([square] * 7),
            pltpu.VMEM((order, order), jnp.float32),
            pltpu.SemaphoreType.DMA((2,)),
            pltpu.SemaphoreType.DMA((order // tile,)),
        ],
        cost_estimate=pl.CostEstimate(
            flops=10 * 2 * order**3, transcendentals=0, bytes_accessed=6 * 2**20
        ),
        compiler_params=pltpu.CompilerParams(vmem_limit_bytes=44 * 2**20),
        name="roots",
    )(mean, due, place, grad, chosen, left_stat, right_stat)


def per_device(grad_parts, left_stat, right_stat, left_root, right_root, due):
    row_count = left_stat.shape[1]
    row_start = lax.axis_index(DP) * row_count
    chosen = choose(due, left_stat[0], right_stat[0], left_root[0], right_root[0])
    chosen = lax.all_gather(chosen, DP, axis=1, tiled=True)
    chosen = pltpu.with_memory_space_constraint(chosen, pltpu.HBM)

    rows = exchange_sum(exchange_sum(grad_parts[0, 0], WIDE), NARROW)
    chunk = spread(rows, NARROW)
    squares = jnp.sum(rows.astype(jnp.float32) ** 2)
    squares = lax.psum(squares, (*DP, *MP))
    grad = spread(chunk, WIDE)
    place = row_start.astype(jnp.int32).reshape(1)
    update, left_new, right_new, left_out, right_out = refs[7:12]
    picked, flipped, first, second, mixed, used, x, fourth, block, sems, sent = refs[12:]
    order = grad.shape[0]
    rows = left_stat.shape[0]
    weight = (1.0 - decay) / order
    columns = [slice(n * tile, (n + 1) * tile) for n in range(order // tile)]
    fetches = [
        pltpu.make_async_copy(chosen.at[k], picked.at[k], sems.at[k]) for k in range(2)
    ]
    for fetch in fetches:
        fetch.start()
    mine = pl.ds(pl.multiple_of(place[0], rows), rows)
    across = ((1,), (0,))
    block_squares = jnp.sum(sums[:, place[1]], 0)[:1]
    squares = jnp.sum(jnp.sum(sums[...], 0), 0)[:1]
    count = float(sums.shape[1] * order * order)
    factor = jnp.broadcast_to(lax.rsqrt(squares / count + epsilon)[:, :1], (1, tile))

    def scale_of(k):
        row = lax.broadcasted_iota(jnp.int32, (128, 128), 0)
        col = lax.broadcasted_iota(jnp.int32, (128, 128), 1)
        diagonal = jnp.zeros((128, 128), jnp.float32)
        for i in range(0, order, 128):
            part = picked[k, i : i + 128, i : i + 128].astype(jnp.float32)
            diagonal = diagonal + jnp.where(row == col, part, 0.0)
        return (4.0 / order) * (decay * jnp.sum(diagonal) + weight * squares)

    def root_of(k, stat, new, out):
        scale_c = jnp.zeros((1, 128), jnp.float32)
        shrink = lift = None
        for n, cols in enumerate(columns):
            if k == 0:
                product = dot(grad[...], grad[cols, :], ((1,), (1,)))
            else:
                product = dot(flipped[...], grad[:, cols], across)
            if n == 0:
                fetches[k].wait()
                scale_c = scale_c + scale_of(k)
                shrink = jnp.broadcast_to((0.25 / scale_c)[:, :1], (1, tile))
                lift = 0.25 * jnp.exp(-0.25 * jnp.log(scale_c))
                lift = jnp.broadcast_to(lift[:, :1], (1, tile))
            block[:, cols] = product
            row = lax.broadcasted_iota(jnp.int32, (order, tile), 0)
            col = n * tile + lax.broadcasted_iota(jnp.int32, (order, tile), 1)
            statistic = decay * picked[k, :, cols].astype(jnp.float32) + weight * product
            first[:, cols] = (jnp.where(row == col, 1.25, 0.0) - statistic * shrink).astype(
                jnp.bfloat16
            )
        new[...] = stat[...] * decay + block[mine, :] * weight
        for cols in columns:
            square = dot(first[...], first[:, cols], across).astype(jnp.bfloat16)
            second[:, cols] = square
            mixed[:, cols] = (
                5.0 * first[:, cols].astype(jnp.float32) - 4.0 * square.astype(jnp.float32)
            ).astype(jnp.bfloat16)
            if k == 0:
                flipped[cols, :] = grad[:, cols].T
        for cols in columns:
            fourth[:, cols] = dot(second[...], second[:, cols], across).astype(jnp.bfloat16)
        for cols in columns:
            inner = dot(fourth[...], mixed[:, cols], across)
            root = lift * (5.0 * first[:, cols].astype(jnp.float32) - inner)
            used[:, cols] = jnp.where(
                due[0, k] == 1, root.astype(jnp.bfloat16), picked[k, :, cols]
            )
        out[...] = used[mine, :]

    root_of(0, left_stat, left_new, left_out)
    for cols in columns:
        x[:, cols] = dot(used[...], grad[:, cols], across).astype(jnp.bfloat16)
    root_of(1, right_stat, right_new, right_out)
    sends = []
    for n, cols in enumerate(columns):
        fourth[:, cols] = (dot(x[...], used[:, cols], across) * factor).astype(jnp.bfloat16)
        sends.append(
            pltpu.make_async_copy(fourth.at[:, cols], update.at[0, :, cols], sent.at[n])
        )
        sends[-1].start()
    for send in sends:
        send.wait()


def roots(mean, due, place, grad, chosen, left_stat, right_stat):
    order = grad.shape[0]
    tile = 512
    new = jax.ShapeDtypeStruct(left_stat.shape, jnp.float32)
    out = jax.ShapeDtypeStruct(left_stat.shape, jnp.bfloat16)
    scalar = pl.BlockSpec(memory_space=pltpu.SMEM)
    vector = pl.BlockSpec(memory_space=pltpu.VMEM)
    far = pl.BlockSpec(memory_space=pltpu.HBM)
    square = pltpu.VMEM((order, order), jnp.bfloat16)
    return pl.pallas_call(
        functools.partial(roots_kernel, tile),
        out_shape=(jax.ShapeDtypeStruct((1, order, order), jnp.bfloat16), new, new, out, out),
        in_specs=[scalar, scalar, scalar, vector, far, vector, vector],
        out_specs=(far, vector, vector, vector, vector),
        scratch_shapes=[
            pltpu.VMEM((2, order, order), jnp.bfloat16),
            *([square] * 7),
            pltpu.VMEM((order, order), jnp.float32),
            pltpu.SemaphoreType.DMA((2,)),
            pltpu.SemaphoreType.DMA((order // tile,)),
        ],
        cost_estimate=pl.CostEstimate(
            flops=10 * 2 * order**3, transcendentals=0, bytes_accessed=6 * 2**20
        ),
        compiler_params=pltpu.CompilerParams(vmem_limit_bytes=44 * 2**20),
        name="roots",
    )(mean, due, place, grad, chosen, left_stat, right_stat)


def per_device(grad_parts, left_stat, right_stat, left_root, right_root, due):
    row_count = left_stat.shape[1]
    row_start = lax.axis_index(DP) * row_count
    chosen = choose(due, left_stat[0], right_stat[0], left_root[0], right_root[0])
    chosen = lax.all_gather(chosen, DP, axis=1, tiled=True)
    chosen = pltpu.with_memory_space_constraint(chosen, pltpu.HBM)

    rows = exchange_sum(exchange_sum(grad_parts[0, 0], WIDE), NARROW)
    chunk = spread(rows, NARROW)
    squares = jnp.sum(rows.astype(jnp.float32) ** 2)
    squares = lax.psum(squares, (*DP, *MP))
    mean = squares / float(lax.axis_size(MP) * left_stat.shape[-1] ** 2)
    grad = spread(chunk, WIDE)
    mean = mean.reshape(1, 1)
    place = jnp.stack([row_start, lax.axis_index(MP)]).astype(jnp.int32)
    update, left_new, right_new, left_out, right_out = roots(
        mean, due, place, grad, chosen, left_stat[0], right_stat[0]
    )
    return (update, left_new[None], right_new[None], left_out[None], right_out[None])


def solution(mesh):
    torus = Mesh(mesh.devices.reshape(4, 4, 2, 4, 2), ("y", "zh", "zl", "x", "c"))
    in_specs = (
        P(DP, MP, None, None),
        P(MP, DP, None),
        P(MP, DP, None),
        P(MP, DP, None),
        P(MP, DP, None),
        P(MP, None),
    )
    out_specs = (
        P(MP, None, None),
        P(MP, DP, None),
        P(MP, DP, None),
        P(MP, DP, None),
        P(MP, DP, None),
    )
    return jax.shard_map(
        per_device, mesh=torus, in_specs=in_specs, out_specs=out_specs, check_vma=False
    )
```

```python
import functools

import jax
import jax.numpy as jnp
from jax import lax
from jax.experimental import pallas as pl
from jax.experimental.pallas import tpu as pltpu
from jax.sharding import Mesh
from jax.sharding import PartitionSpec as P

DP = ("y", "zh", "zl")
MP = ("x", "c")
WIDE = ("y", "zl")
NARROW = "zh"

epsilon = 1e-06
decay = 0.9


def dot(a, b, dims):
    return lax.dot_general(a, b, (dims, ((), ())), preferred_element_type=jnp.float32)


def exchange_sum(value, axes):
    groups = lax.axis_size(axes)
    parts = value.reshape(groups, value.shape[0] // groups, value.shape[1])
    parts = lax.all_to_all(parts, axes, 0, 0, tiled=True)
    return jnp.sum(parts.astype(jnp.float32), 0).astype(jnp.bfloat16)


def spread(value, axes):
    groups = lax.axis_size(axes)
    copies = jnp.broadcast_to(value[None], (groups, *value.shape))
    parts = lax.all_to_all(copies, axes, 0, 0, tiled=True)
    return parts.reshape(groups * value.shape[0], value.shape[1])


def sum_of_four(value, axes):
    others = []
    for mask in (1, 2, 3):
        swap = [(i, i ^ mask) for i in range(4)]
        others.append(lax.ppermute(value, axes, swap))
    return (value + others[0]) + (others[1] + others[2])


def choose_kernel(due, left_stat, right_stat, left_root, right_root, chosen):
    for k, stat, root in ((0, left_stat, left_root), (1, right_stat, right_root)):
        chosen[k] = jnp.where(due[0, k] == 1, stat[...].astype(jnp.bfloat16), root[...])


def choose(due, left_stat, right_stat, left_root, right_root):
    vector = pl.BlockSpec(memory_space=pltpu.VMEM)
    return pl.pallas_call(
        choose_kernel,
        out_shape=jax.ShapeDtypeStruct((2, *left_root.shape), jnp.bfloat16),
        in_specs=[pl.BlockSpec(memory_space=pltpu.SMEM), vector, vector, vector, vector],
        out_specs=vector,
        compiler_params=pltpu.CompilerParams(vmem_limit_bytes=4 * 2**20),
        name="choose",
    )(due, left_stat, right_stat, left_root, right_root)


def roots_kernel(tile, blocks, *refs):
    total, due, place, grad, chosen, left_stat, right_stat = refs[:7]
    update, left_new, right_new, left_out, right_out = refs[7:12]
    picked, flipped, first, second, mixed, used, x, fourth, block, sems, sent = refs[12:]
    order = grad.shape[0]
    rows = left_stat.shape[0]
    weight = (1.0 - decay) / order
    columns = [slice(n * tile, (n + 1) * tile) for n in range(order // tile)]
    fetches = [
        pltpu.make_async_copy(chosen.at[k], picked.at[k], sems.at[k]) for k in range(2)
    ]
    for fetch in fetches:
        fetch.start()
    mine = pl.ds(pl.multiple_of(place[0], rows), rows)
    across = ((1,), (0,))
    factor = lax.rsqrt(total[:1] / float(blocks * order * order) + epsilon)
    factor = jnp.broadcast_to(factor[:, :1], (1, tile))

    def energy():
        partial = jnp.zeros((128, order), jnp.float32)
        for i in range(0, order, 128):
            part = grad[i : i + 128, :].astype(jnp.float32)
            partial = partial + part * part
        return jnp.sum(partial)

    squares = energy()

    def scale_of(k):
        row = lax.broadcasted_iota(jnp.int32, (128, 128), 0)
        col = lax.broadcasted_iota(jnp.int32, (128, 128), 1)
        diagonal = jnp.zeros((128, 128), jnp.float32)
        for i in range(0, order, 128):
            part = picked[k, i : i + 128, i : i + 128].astype(jnp.float32)
            diagonal = diagonal + jnp.where(row == col, part, 0.0)
        return (4.0 / order) * (decay * jnp.sum(diagonal) + weight * squares)

    def root_of(k, stat, new, out):
        scale_c = jnp.zeros((1, 128), jnp.float32)
        shrink = lift = None
        for n, cols in enumerate(columns):
            if k == 0:
                product = dot(grad[...], grad[cols, :], ((1,), (1,)))
            else:
                product = dot(flipped[...], grad[:, cols], across)
            if n == 0:
                fetches[k].wait()
                scale_c = scale_c + scale_of(k)
                shrink = jnp.broadcast_to((0.25 / scale_c)[:, :1], (1, tile))
                lift = 0.25 * jnp.exp(-0.25 * jnp.log(scale_c))
                lift = jnp.broadcast_to(lift[:, :1], (1, tile))
            block[:, cols] = product
            row = lax.broadcasted_iota(jnp.int32, (order, tile), 0)
            col = n * tile + lax.broadcasted_iota(jnp.int32, (order, tile), 1)
            statistic = decay * picked[k, :, cols].astype(jnp.float32) + weight * product
            first[:, cols] = (jnp.where(row == col, 1.25, 0.0) - statistic * shrink).astype(
                jnp.bfloat16
            )
        new[...] = stat[...] * decay + block[mine, :] * weight
        for cols in columns:
            square = dot(first[...], first[:, cols], across).astype(jnp.bfloat16)
            second[:, cols] = square
            mixed[:, cols] = (
                5.0 * first[:, cols].astype(jnp.float32) - 4.0 * square.astype(jnp.float32)
            ).astype(jnp.bfloat16)
            if k == 0:
                flipped[cols, :] = grad[:, cols].T
        for cols in columns:
            fourth[:, cols] = dot(second[...], second[:, cols], across).astype(jnp.bfloat16)
        for cols in columns:
            inner = dot(fourth[...], mixed[:, cols], across)
            root = lift * (5.0 * first[:, cols].astype(jnp.float32) - inner)
            used[:, cols] = jnp.where(
                due[0, k] == 1, root.astype(jnp.bfloat16), picked[k, :, cols]
            )
        out[...] = used[mine, :]

    root_of(0, left_stat, left_new, left_out)
    for cols in columns:
        x[:, cols] = dot(used[...], grad[:, cols], across).astype(jnp.bfloat16)
    root_of(1, right_stat, right_new, right_out)
    sends = []
    for n, cols in enumerate(columns):
        fourth[:, cols] = (dot(x[...], used[:, cols], across) * factor).astype(jnp.bfloat16)
        sends.append(
            pltpu.make_async_copy(fourth.at[:, cols], update.at[0, :, cols], sent.at[n])
        )
        sends[-1].start()
    for send in sends:
        send.wait()


def roots(total, due, place, grad, chosen, left_stat, right_stat):
    order = grad.shape[0]
    tile = 512
    new = jax.ShapeDtypeStruct(left_stat.shape, jnp.float32)
    out = jax.ShapeDtypeStruct(left_stat.shape, jnp.bfloat16)
    scalar = pl.BlockSpec(memory_space=pltpu.SMEM)
    vector = pl.BlockSpec(memory_space=pltpu.VMEM)
    far = pl.BlockSpec(memory_space=pltpu.HBM)
    square = pltpu.VMEM((order, order), jnp.bfloat16)
    return pl.pallas_call(
        functools.partial(roots_kernel, tile, lax.axis_size(MP)),
        out_shape=(jax.ShapeDtypeStruct((1, order, order), jnp.bfloat16), new, new, out, out),
        in_specs=[vector, scalar, scalar, vector, far, vector, vector],
        out_specs=(far, vector, vector, vector, vector),
        scratch_shapes=[
            pltpu.VMEM((2, order, order), jnp.bfloat16),
            *([square] * 7),
            pltpu.VMEM((order, order), jnp.float32),
            pltpu.SemaphoreType.DMA((2,)),
            pltpu.SemaphoreType.DMA((order // tile,)),
        ],
        cost_estimate=pl.CostEstimate(
            flops=10 * 2 * order**3, transcendentals=0, bytes_accessed=6 * 2**20
        ),
        compiler_params=pltpu.CompilerParams(vmem_limit_bytes=44 * 2**20),
        name="roots",
    )(total, due, place, grad, chosen, left_stat, right_stat)


def per_device(grad_parts, left_stat, right_stat, left_root, right_root, due):
    row_count = left_stat.shape[1]
    row_start = lax.axis_index(DP) * row_count
    chosen = choose(due, left_stat[0], right_stat[0], left_root[0], right_root[0])
    chosen = lax.all_gather(chosen, DP, axis=1, tiled=True)
    chosen = pltpu.with_memory_space_constraint(chosen, pltpu.HBM)

    rows = exchange_sum(exchange_sum(grad_parts[0, 0], WIDE), NARROW)
    chunk = spread(rows, NARROW)
    squares = jnp.sum(chunk.astype(jnp.float32) ** 2)
    total = jnp.full((8, 128), squares, jnp.float32)
    for axes in (("zl", "c"), ("x",), ("y",)):
        total = sum_of_four(total, axes)
    grad = spread(chunk, WIDE)
    place = row_start.astype(jnp.int32).reshape(1)
    update, left_new, right_new, left_out, right_out = roots(
        total, due, place, grad, chosen, left_stat[0], right_stat[0]
    )
    return (update, left_new[None], right_new[None], left_out[None], right_out[None])


def solution(mesh):
    torus = Mesh(mesh.devices.reshape(4, 4, 2, 4, 2), ("y", "zh", "zl", "x", "c"))
    in_specs = (
        P(DP, MP, None, None),
        P(MP, DP, None),
        P(MP, DP, None),
        P(MP, DP, None),
        P(MP, DP, None),
        P(MP, None),
    )
    out_specs = (
        P(MP, None, None),
        P(MP, DP, None),
        P(MP, DP, None),
        P(MP, DP, None),
        P(MP, DP, None),
    )
    return jax.shard_map(
        per_device, mesh=torus, in_specs=in_specs, out_specs=out_specs, check_vma=False
    )
```

```python
import functools

import jax
import jax.numpy as jnp
from jax import lax
from jax.experimental import pallas as pl
from jax.experimental.pallas import tpu as pltpu
from jax.sharding import Mesh
from jax.sharding import PartitionSpec as P

DP = ("y", "zh", "zl")
MP = ("x", "c")
WIDE = ("y", "zl")
NARROW = "zh"

epsilon = 1e-06
decay = 0.9


def dot(a, b, dims):
    return lax.dot_general(a, b, (dims, ((), ())), preferred_element_type=jnp.float32)


def exchange_sum(value, axes):
    groups = lax.axis_size(axes)
    parts = value.reshape(groups, value.shape[0] // groups, value.shape[1])
    parts = lax.all_to_all(parts, axes, 0, 0, tiled=True)
    return jnp.sum(parts.astype(jnp.float32), 0).astype(jnp.bfloat16)


def spread(value, axes):
    groups = lax.axis_size(axes)
    copies = jnp.broadcast_to(value[None], (groups, *value.shape))
    parts = lax.all_to_all(copies, axes, 0, 0, tiled=True)
    return parts.reshape(groups * value.shape[0], value.shape[1])


def sum_over(value, axes):
    size = lax.axis_size(axes)
    parts = [value]
    for mask in range(1, size):
        swap = [(i, i ^ mask) for i in range(size)]
        parts.append(lax.ppermute(value, axes, swap))
    while len(parts) > 1:
        parts = [a + b for a, b in zip(parts[::2], parts[1::2])]
    return parts[0]


def choose_kernel(due, left_stat, right_stat, left_root, right_root, chosen, *scratch):
    flags, *held, sems = scratch
    far = (due, left_stat, right_stat, left_root, right_root)
    fetches = [
        pltpu.make_async_copy(ref, near, sems.at[i])
        for i, (ref, near) in enumerate(zip(far, (flags, *held)))
    ]
    for fetch in fetches:
        fetch.start()
    for fetch in fetches:
        fetch.wait()
    for k in range(2):
        stat, root = held[k][...], held[2 + k][...]
        chosen[k] = jnp.where(flags[0, k] == 1, stat.astype(jnp.bfloat16), root)


def choose(*arrays):
    far = pl.BlockSpec(memory_space=pltpu.HBM)
    arrays = [pltpu.with_memory_space_constraint(a, pltpu.HBM) for a in arrays]
    due, *rows = arrays
    root = rows[-1]
    return pl.pallas_call(
        choose_kernel,
        out_shape=jax.ShapeDtypeStruct((2, *root.shape), root.dtype),
        in_specs=[far] * len(arrays),
        out_specs=pl.BlockSpec(memory_space=pltpu.VMEM),
        scratch_shapes=[
            pltpu.SMEM(due.shape, due.dtype),
            *[pltpu.VMEM(a.shape, a.dtype) for a in rows],
            pltpu.SemaphoreType.DMA((len(arrays),)),
        ],
        compiler_params=pltpu.CompilerParams(vmem_limit_bytes=4 * 2**20),
        name="choose",
    )(*arrays)


def roots_kernel(tile, blocks, *refs):
    total, due, place, grad, chosen, left_stat, right_stat = refs[:7]
    update, left_new, right_new, left_out, right_out = refs[7:12]
    picked, flipped, first, second, mixed, used, x, fourth, block, sems, sent = refs[12:]
    order = grad.shape[0]
    rows = left_stat.shape[0]
    weight = (1.0 - decay) / order
    columns = [slice(n * tile, (n + 1) * tile) for n in range(order // tile)]
    fetches = [
        pltpu.make_async_copy(chosen.at[k], picked.at[k], sems.at[k]) for k in range(2)
    ]
    for fetch in fetches:
        fetch.start()
    mine = pl.ds(pl.multiple_of(place[0], rows), rows)
    across = ((1,), (0,))
    factor = lax.rsqrt(total[:1] / float(blocks * order * order) + epsilon)
    factor = jnp.broadcast_to(factor[:, :1], (1, tile))

    def energy():
        partial = jnp.zeros((128, order), jnp.float32)
        for i in range(0, order, 128):
            part = grad[i : i + 128, :].astype(jnp.float32)
            partial = partial + part * part
        return jnp.sum(partial)

    squares = energy()

    def scale_of(k):
        row = lax.broadcasted_iota(jnp.int32, (128, 128), 0)
        col = lax.broadcasted_iota(jnp.int32, (128, 128), 1)
        diagonal = jnp.zeros((128, 128), jnp.float32)
        for i in range(0, order, 128):
            part = picked[k, i : i + 128, i : i + 128].astype(jnp.float32)
            diagonal = diagonal + jnp.where(row == col, part, 0.0)
        return (4.0 / order) * (decay * jnp.sum(diagonal) + weight * squares)

    def root_of(k, stat, new, out):
        scale_c = jnp.zeros((1, 128), jnp.float32)
        shrink = lift = None
        for n, cols in enumerate(columns):
            if k == 0:
                product = dot(grad[...], grad[cols, :], ((1,), (1,)))
            else:
                product = dot(flipped[...], grad[:, cols], across)
            if n == 0:
                fetches[k].wait()
                scale_c = scale_c + scale_of(k)
                shrink = jnp.broadcast_to((0.25 / scale_c)[:, :1], (1, tile))
                lift = 0.25 * jnp.exp(-0.25 * jnp.log(scale_c))
                lift = jnp.broadcast_to(lift[:, :1], (1, tile))
            block[:, cols] = product
            row = lax.broadcasted_iota(jnp.int32, (order, tile), 0)
            col = n * tile + lax.broadcasted_iota(jnp.int32, (order, tile), 1)
            statistic = decay * picked[k, :, cols].astype(jnp.float32) + weight * product
            first[:, cols] = (jnp.where(row == col, 1.25, 0.0) - statistic * shrink).astype(
                jnp.bfloat16
            )
        new[...] = stat[...] * decay + block[mine, :] * weight
        for cols in columns:
            square = dot(first[...], first[:, cols], across).astype(jnp.bfloat16)
            second[:, cols] = square
            mixed[:, cols] = (
                5.0 * first[:, cols].astype(jnp.float32) - 4.0 * square.astype(jnp.float32)
            ).astype(jnp.bfloat16)
            if k == 0:
                flipped[cols, :] = grad[:, cols].T
        for cols in columns:
            fourth[:, cols] = dot(second[...], second[:, cols], across).astype(jnp.bfloat16)
        for cols in columns:
            inner = dot(fourth[...], mixed[:, cols], across)
            root = lift * (5.0 * first[:, cols].astype(jnp.float32) - inner)
            used[:, cols] = jnp.where(
                due[0, k] == 1, root.astype(jnp.bfloat16), picked[k, :, cols]
            )
        out[...] = used[mine, :]

    root_of(0, left_stat, left_new, left_out)
    for cols in columns:
        x[:, cols] = dot(used[...], grad[:, cols], across).astype(jnp.bfloat16)
    root_of(1, right_stat, right_new, right_out)
    sends = []
    for n, cols in enumerate(columns):
        fourth[:, cols] = (dot(x[...], used[:, cols], across) * factor).astype(jnp.bfloat16)
        sends.append(
            pltpu.make_async_copy(fourth.at[:, cols], update.at[0, :, cols], sent.at[n])
        )
        sends[-1].start()
    for send in sends:
        send.wait()


def roots(total, due, place, grad, chosen, left_stat, right_stat):
    order = grad.shape[0]
    tile = 512
    new = jax.ShapeDtypeStruct(left_stat.shape, jnp.float32)
    out = jax.ShapeDtypeStruct(left_stat.shape, jnp.bfloat16)
    scalar = pl.BlockSpec(memory_space=pltpu.SMEM)
    vector = pl.BlockSpec(memory_space=pltpu.VMEM)
    far = pl.BlockSpec(memory_space=pltpu.HBM)
    square = pltpu.VMEM((order, order), jnp.bfloat16)
    return pl.pallas_call(
        functools.partial(roots_kernel, tile, lax.axis_size(MP)),
        out_shape=(jax.ShapeDtypeStruct((1, order, order), jnp.bfloat16), new, new, out, out),
        in_specs=[vector, scalar, scalar, vector, far, vector, vector],
        out_specs=(far, vector, vector, vector, vector),
        scratch_shapes=[
            pltpu.VMEM((2, order, order), jnp.bfloat16),
            *([square] * 7),
            pltpu.VMEM((order, order), jnp.float32),
            pltpu.SemaphoreType.DMA((2,)),
            pltpu.SemaphoreType.DMA((order // tile,)),
        ],
        cost_estimate=pl.CostEstimate(
            flops=10 * 2 * order**3, transcendentals=0, bytes_accessed=6 * 2**20
        ),
        compiler_params=pltpu.CompilerParams(vmem_limit_bytes=44 * 2**20),
        name="roots",
    )(total, due, place, grad, chosen, left_stat, right_stat)


def per_device(grad_parts, left_stat, right_stat, left_root, right_root, due):
    row_count = left_stat.shape[1]
    row_start = lax.axis_index(DP) * row_count
    chosen = choose(due, left_stat[0], right_stat[0], left_root[0], right_root[0])
    chosen, partial = lax.optimization_barrier((chosen, grad_parts[0, 0]))
    chosen = lax.all_gather(chosen, DP, axis=1, tiled=True)
    chosen = pltpu.with_memory_space_constraint(chosen, pltpu.HBM)

    part = exchange_sum(partial, WIDE)
    rows = exchange_sum(part, NARROW)
    chunk = spread(rows, NARROW)
    squares = jnp.sum(chunk.astype(jnp.float32) ** 2)
    total = jnp.full((8, 128), squares, jnp.float32)
    for axes in ("c", "x", WIDE):
        total = sum_over(total, axes)
    grad = spread(chunk, WIDE)
    place = row_start.astype(jnp.int32).reshape(1)
    update, left_new, right_new, left_out, right_out = roots(
        total, due, place, grad, chosen, left_stat[0], right_stat[0]
    )
    return (update, left_new[None], right_new[None], left_out[None], right_out[None])


def solution(mesh):
    torus = Mesh(mesh.devices.reshape(4, 4, 2, 4, 2), ("y", "zh", "zl", "x", "c"))
    in_specs = (
        P(DP, MP, None, None),
        P(MP, DP, None),
        P(MP, DP, None),
        P(MP, DP, None),
        P(MP, DP, None),
        P(MP, None),
    )
    out_specs = (
        P(MP, None, None),
        P(MP, DP, None),
        P(MP, DP, None),
        P(MP, DP, None),
        P(MP, DP, None),
    )
    return jax.shard_map(
        per_device, mesh=torus, in_specs=in_specs, out_specs=out_specs, check_vma=False
    )
```

```python
import functools

import jax
import jax.numpy as jnp
from jax import lax
from jax.experimental import pallas as pl
from jax.experimental.pallas import tpu as pltpu
from jax.sharding import Mesh
from jax.sharding import PartitionSpec as P

DP = ("y", "zh", "zl")
MP = ("x", "c")
WIDE = ("y", "zl")
NARROW = "zh"

epsilon = 1e-06
decay = 0.9


def dot(a, b, dims):
    return lax.dot_general(a, b, (dims, ((), ())), preferred_element_type=jnp.float32)


def exchange_sum(value, axes):
    groups = lax.axis_size(axes)
    parts = value.reshape(groups, value.shape[0] // groups, value.shape[1])
    parts = lax.all_to_all(parts, axes, 0, 0, tiled=True)
    return jnp.sum(parts.astype(jnp.float32), 0).astype(jnp.bfloat16)


def spread(value, axes):
    groups = lax.axis_size(axes)
    copies = jnp.broadcast_to(value[None], (groups, *value.shape))
    parts = lax.all_to_all(copies, axes, 0, 0, tiled=True)
    return parts.reshape(groups * value.shape[0], value.shape[1])


def sum_over(value, axes):
    size = lax.axis_size(axes)
    parts = [value]
    for mask in range(1, size):
        swap = [(i, i ^ mask) for i in range(size)]
        parts.append(lax.ppermute(value, axes, swap))
    while len(parts) > 1:
        parts = [a + b for a, b in zip(parts[::2], parts[1::2])]
    return parts[0]


def choose_kernel(due, left_stat, right_stat, left_root, right_root, chosen, *scratch):
    flags, *held, sems = scratch
    far = (due, left_stat, right_stat, left_root, right_root)
    fetches = [
        pltpu.make_async_copy(ref, near, sems.at[i])
        for i, (ref, near) in enumerate(zip(far, (flags, *held)))
    ]
    for fetch in fetches:
        fetch.start()
    for fetch in fetches:
        fetch.wait()
    for k in range(2):
        stat, root = held[k][...], held[2 + k][...]
        chosen[k] = jnp.where(flags[0, k] == 1, stat.astype(jnp.bfloat16), root)


def choose(*arrays):
    far = pl.BlockSpec(memory_space=pltpu.HBM)
    arrays = [pltpu.with_memory_space_constraint(a, pltpu.HBM) for a in arrays]
    due, *rows = arrays
    root = rows[-1]
    return pl.pallas_call(
        choose_kernel,
        out_shape=jax.ShapeDtypeStruct((2, *root.shape), root.dtype),
        in_specs=[far] * len(arrays),
        out_specs=pl.BlockSpec(memory_space=pltpu.VMEM),
        scratch_shapes=[
            pltpu.SMEM(due.shape, due.dtype),
            *[pltpu.VMEM(a.shape, a.dtype) for a in rows],
            pltpu.SemaphoreType.DMA((len(arrays),)),
        ],
        compiler_params=pltpu.CompilerParams(vmem_limit_bytes=4 * 2**20),
        name="choose",
    )(*arrays)


def roots_kernel(tile, blocks, *refs):
    total, due, place, grad, chosen, left_stat, right_stat = refs[:7]
    update, left_new, right_new, left_out, right_out = refs[7:12]
    picked, flipped, first, second, mixed, used, x, fourth, block = refs[12:21]
    new_rows, out_rows, sems, sent = refs[21:]
    sends = []

    def send(source, target):
        sends.append(pltpu.make_async_copy(source, target, sent.at[len(sends)]))
        sends[-1].start()

    order = grad.shape[0]
    rows = left_stat.shape[0]
    weight = (1.0 - decay) / order
    columns = [slice(n * tile, (n + 1) * tile) for n in range(order // tile)]
    step = 256
    corners = [
        (slice(i, order), slice(i, i + step), slice(i + step, order))
        for i in range(0, order, step)
    ]
    fetches = [
        pltpu.make_async_copy(chosen.at[k], picked.at[k], sems.at[k]) for k in range(2)
    ]
    for fetch in fetches:
        fetch.start()
    mine = pl.ds(pl.multiple_of(place[0], rows), rows)
    across = ((1,), (0,))
    factor = lax.rsqrt(total[:1] / float(blocks * order * order) + epsilon)
    factor = jnp.broadcast_to(factor[:, :1], (1, tile))

    def energy():
        partial = jnp.zeros((128, order), jnp.float32)
        for i in range(0, order, 128):
            part = grad[i : i + 128, :].astype(jnp.float32)
            partial = partial + part * part
        return jnp.sum(partial)

    squares = energy()

    def scale_of(k):
        row = lax.broadcasted_iota(jnp.int32, (128, 128), 0)
        col = lax.broadcasted_iota(jnp.int32, (128, 128), 1)
        diagonal = jnp.zeros((128, 128), jnp.float32)
        for i in range(0, order, 128):
            part = picked[k, i : i + 128, i : i + 128].astype(jnp.float32)
            diagonal = diagonal + jnp.where(row == col, part, 0.0)
        return (4.0 / order) * (decay * jnp.sum(diagonal) + weight * squares)

    def root_of(k, stat, new, out):
        scale_c = jnp.zeros((1, 128), jnp.float32)
        shrink = lift = None
        for n, cols in enumerate(columns):
            if k == 0:
                product = dot(grad[...], grad[cols, :], ((1,), (1,)))
            else:
                product = dot(flipped[...], grad[:, cols], across)
            if n == 0:
                fetches[k].wait()
                scale_c = scale_c + scale_of(k)
                shrink = jnp.broadcast_to((0.25 / scale_c)[:, :1], (1, tile))
                lift = 0.25 * jnp.exp(-0.25 * jnp.log(scale_c))
                lift = jnp.broadcast_to(lift[:, :1], (1, tile))
            block[:, cols] = product
            row = lax.broadcasted_iota(jnp.int32, (order, tile), 0)
            col = n * tile + lax.broadcasted_iota(jnp.int32, (order, tile), 1)
            statistic = decay * picked[k, :, cols].astype(jnp.float32) + weight * product
            first[:, cols] = (jnp.where(row == col, 1.25, 0.0) - statistic * shrink).astype(
                jnp.bfloat16
            )
        new_rows[k] = stat[...] * decay + block[mine, :] * weight
        send(new_rows.at[k], new)
        if k == 0:
            for cols in columns:
                flipped[cols, :] = grad[:, cols].T
        for rest, cols, beyond in corners:
            square = dot(first[rest, :], first[:, cols], across).astype(jnp.bfloat16)
            second[rest, cols] = square
            parts = [(rest, cols)]
            if beyond.start < order:
                second[cols, beyond] = square[step:].T
                parts.append((cols, beyond))
            for here, there in parts:
                mixed[here, there] = (
                    5.0 * first[here, there].astype(jnp.float32)
                    - 4.0 * second[here, there].astype(jnp.float32)
                ).astype(jnp.bfloat16)
        for rest, cols, beyond in corners:
            power = dot(second[rest, :], second[:, cols], across).astype(jnp.bfloat16)
            fourth[rest, cols] = power
            if beyond.start < order:
                fourth[cols, beyond] = power[step:].T
        for rest, cols, beyond in corners:
            inner = dot(fourth[rest, :], mixed[:, cols], across)
            root = lift[:, :step] * (5.0 * first[rest, cols].astype(jnp.float32) - inner)
            root = root.astype(jnp.bfloat16)
            used[rest, cols] = jnp.where(due[0, k] == 1, root, picked[k, rest, cols])
            if beyond.start < order:
                flip = root[step:].T
                used[cols, beyond] = jnp.where(due[0, k] == 1, flip, picked[k, cols, beyond])
        out_rows[k] = used[mine, :]
        send(out_rows.at[k], out)

    root_of(0, left_stat, left_new, left_out)
    for cols in columns:
        x[:, cols] = dot(used[...], grad[:, cols], across).astype(jnp.bfloat16)
    root_of(1, right_stat, right_new, right_out)
    for start in range(0, order, 256):
        cols = slice(start, start + 256)
        scaled = dot(x[...], used[:, cols], across) * factor[:, :256]
        fourth[:, cols] = scaled.astype(jnp.bfloat16)
        send(fourth.at[:, cols], update.at[0, :, cols])
    for copy in sends:
        copy.wait()


def roots(total, due, place, grad, chosen, left_stat, right_stat):
    order = grad.shape[0]
    tile = 512
    new = jax.ShapeDtypeStruct(left_stat.shape, jnp.float32)
    out = jax.ShapeDtypeStruct(left_stat.shape, jnp.bfloat16)
    scalar = pl.BlockSpec(memory_space=pltpu.SMEM)
    vector = pl.BlockSpec(memory_space=pltpu.VMEM)
    far = pl.BlockSpec(memory_space=pltpu.HBM)
    square = pltpu.VMEM((order, order), jnp.bfloat16)
    return pl.pallas_call(
        functools.partial(roots_kernel, tile, lax.axis_size(MP)),
        out_shape=(jax.ShapeDtypeStruct((1, order, order), jnp.bfloat16), new, new, out, out),
        in_specs=[vector, scalar, scalar, vector, far, vector, vector],
        out_specs=(far,) * 5,
        scratch_shapes=[
            pltpu.VMEM((2, order, order), jnp.bfloat16),
            *([square] * 7),
            pltpu.VMEM((order, order), jnp.float32),
            pltpu.VMEM((2, *left_stat.shape), jnp.float32),
            pltpu.VMEM((2, *left_stat.shape), jnp.bfloat16),
            pltpu.SemaphoreType.DMA((2,)),
            pltpu.SemaphoreType.DMA((4 + order // 256,)),
        ],
        cost_estimate=pl.CostEstimate(
            flops=10 * 2 * order**3, transcendentals=0, bytes_accessed=6 * 2**20
        ),
        compiler_params=pltpu.CompilerParams(vmem_limit_bytes=44 * 2**20),
        name="roots",
    )(total, due, place, grad, chosen, left_stat, right_stat)


def per_device(grad_parts, left_stat, right_stat, left_root, right_root, due):
    row_count = left_stat.shape[1]
    row_start = lax.axis_index(DP) * row_count
    chosen = choose(due, left_stat[0], right_stat[0], left_root[0], right_root[0])
    chosen, partial = lax.optimization_barrier((chosen, grad_parts[0, 0]))
    chosen = lax.all_gather(chosen, DP, axis=1, tiled=True)
    chosen = pltpu.with_memory_space_constraint(chosen, pltpu.HBM)

    part = exchange_sum(partial, WIDE)
    rows = exchange_sum(part, NARROW)
    chunk = spread(rows, ("zl", "zh"))
    squares = jnp.sum(chunk.astype(jnp.float32) ** 2)
    total = jnp.full((8, 128), squares, jnp.float32)
    for axes in ("c", "x", "y"):
        total = sum_over(total, axes)
    grad = spread(chunk, "y")
    place = row_start.astype(jnp.int32).reshape(1)
    update, left_new, right_new, left_out, right_out = roots(
        total, due, place, grad, chosen, left_stat[0], right_stat[0]
    )
    return (update, left_new[None], right_new[None], left_out[None], right_out[None])


def solution(mesh):
    torus = Mesh(mesh.devices.reshape(4, 4, 2, 4, 2), ("y", "zh", "zl", "x", "c"))
    in_specs = (
        P(DP, MP, None, None),
        P(MP, DP, None),
        P(MP, DP, None),
        P(MP, DP, None),
        P(MP, DP, None),
        P(MP, None),
    )
    out_specs = (
        P(MP, None, None),
        P(MP, DP, None),
        P(MP, DP, None),
        P(MP, DP, None),
        P(MP, DP, None),
    )
    return jax.shard_map(
        per_device, mesh=torus, in_specs=in_specs, out_specs=out_specs, check_vma=False
    )
```

```python
import functools

import jax
import jax.numpy as jnp
from jax import lax
from jax.experimental import pallas as pl
from jax.experimental.pallas import tpu as pltpu
from jax.sharding import Mesh
from jax.sharding import PartitionSpec as P

DP = ("y", "zh", "zl")
MP = ("x", "c")
WIDE = ("y", "zl")
NARROW = "zh"

epsilon = 1e-06
decay = 0.9


def dot(a, b, dims):
    return lax.dot_general(a, b, (dims, ((), ())), preferred_element_type=jnp.float32)


def exchange_sum(value, axes):
    groups = lax.axis_size(axes)
    parts = value.reshape(groups, value.shape[0] // groups, value.shape[1])
    parts = lax.all_to_all(parts, axes, 0, 0, tiled=True)
    return jnp.sum(parts.astype(jnp.float32), 0).astype(jnp.bfloat16)


def spread(value, axes):
    groups = lax.axis_size(axes)
    copies = jnp.broadcast_to(value[None], (groups, *value.shape))
    parts = lax.all_to_all(copies, axes, 0, 0, tiled=True)
    return parts.reshape(groups * value.shape[0], value.shape[1])


def sum_over(value, axes):
    size = lax.axis_size(axes)
    parts = [value]
    for mask in range(1, size):
        swap = [(i, i ^ mask) for i in range(size)]
        parts.append(lax.ppermute(value, axes, swap))
    while len(parts) > 1:
        parts = [a + b for a, b in zip(parts[::2], parts[1::2])]
    return parts[0]


def partner(value, axis, mask):
    swap = [(i, i ^ mask) for i in range(lax.axis_size(axis))]
    return lax.ppermute(value, axis, swap)


def choose_kernel(due, left_stat, right_stat, left_root, right_root, chosen, *scratch):
    flags, *held, sems = scratch
    far = (due, left_stat, right_stat, left_root, right_root)
    fetches = [
        pltpu.make_async_copy(ref, near, sems.at[i])
        for i, (ref, near) in enumerate(zip(far, (flags, *held)))
    ]
    for fetch in fetches:
        fetch.start()
    for fetch in fetches:
        fetch.wait()
    for k in range(2):
        stat, root = held[k][...], held[2 + k][...]
        chosen[k] = jnp.where(flags[0, k] == 1, stat.astype(jnp.bfloat16), root)


def choose(*arrays):
    far = pl.BlockSpec(memory_space=pltpu.HBM)
    arrays = [pltpu.with_memory_space_constraint(a, pltpu.HBM) for a in arrays]
    due, *rows = arrays
    root = rows[-1]
    return pl.pallas_call(
        choose_kernel,
        out_shape=jax.ShapeDtypeStruct((2, *root.shape), root.dtype),
        in_specs=[far] * len(arrays),
        out_specs=pl.BlockSpec(memory_space=pltpu.VMEM),
        scratch_shapes=[
            pltpu.SMEM(due.shape, due.dtype),
            *[pltpu.VMEM(a.shape, a.dtype) for a in rows],
            pltpu.SemaphoreType.DMA((len(arrays),)),
        ],
        compiler_params=pltpu.CompilerParams(vmem_limit_bytes=4 * 2**20),
        name="choose",
    )(*arrays)


def roots_kernel(tile, blocks, *refs):
    total, due, place = refs[:3]
    chunk, next_one, last_one, far_half, far_other, chosen, left_stat, right_stat = refs[3:11]
    update, left_new, right_new, left_out, right_out = refs[11:16]
    picked, grad, flipped, first, second, mixed, used, x, fourth, block = refs[16:26]
    new_rows, out_rows, sems, sent = refs[26:]
    sends = []

    def send(source, target):
        sends.append(pltpu.make_async_copy(source, target, sent.at[len(sends)]))
        sends[-1].start()

    order = chosen.shape[-1]
    rows = left_stat.shape[0]
    weight = (1.0 - decay) / order
    columns = [slice(n * tile, (n + 1) * tile) for n in range(order // tile)]
    step = 256
    corners = [
        (slice(i, order), slice(i, i + step), slice(i + step, order))
        for i in range(0, order, step)
    ]
    fetches = [
        pltpu.make_async_copy(chosen.at[k], picked.at[k], sems.at[k]) for k in range(2)
    ]
    for fetch in fetches:
        fetch.start()
    full, half = chunk.shape[0], far_half.shape[0]
    row, side = place[1], place[2]
    far = (row ^ 2) * full
    for piece, at in (
        (chunk, row * full),
        (next_one, (row ^ 1) * full),
        (last_one, (row ^ 3) * full),
        (far_half, far + side * half),
        (far_other, far + (1 - side) * half),
    ):
        grad[pl.ds(pl.multiple_of(at, half), piece.shape[0]), :] = piece[...]
    mine = pl.ds(pl.multiple_of(place[0], rows), rows)
    across = ((1,), (0,))
    factor = lax.rsqrt(total[:1] / float(blocks * order * order) + epsilon)
    factor = jnp.broadcast_to(factor[:, :1], (1, tile))

    def energy():
        partial = jnp.zeros((128, order), jnp.float32)
        for i in range(0, order, 128):
            part = grad[i : i + 128, :].astype(jnp.float32)
            partial = partial + part * part
        return jnp.sum(partial)

    squares = energy()

    def scale_of(k):
        row = lax.broadcasted_iota(jnp.int32, (128, 128), 0)
        col = lax.broadcasted_iota(jnp.int32, (128, 128), 1)
        diagonal = jnp.zeros((128, 128), jnp.float32)
        for i in range(0, order, 128):
            part = picked[k, i : i + 128, i : i + 128].astype(jnp.float32)
            diagonal = diagonal + jnp.where(row == col, part, 0.0)
        return (4.0 / order) * (decay * jnp.sum(diagonal) + weight * squares)

    def root_of(k, stat, new, out):
        scale_c = jnp.zeros((1, 128), jnp.float32)
        shrink = lift = None
        for n, cols in enumerate(columns):
            if k == 0:
                product = dot(grad[...], grad[cols, :], ((1,), (1,)))
            else:
                product = dot(flipped[...], grad[:, cols], across)
            if n == 0:
                fetches[k].wait()
                scale_c = scale_c + scale_of(k)
                shrink = jnp.broadcast_to((0.25 / scale_c)[:, :1], (1, tile))
                lift = 0.25 * jnp.exp(-0.25 * jnp.log(scale_c))
                lift = jnp.broadcast_to(lift[:, :1], (1, tile))
            block[:, cols] = product
            row = lax.broadcasted_iota(jnp.int32, (order, tile), 0)
            col = n * tile + lax.broadcasted_iota(jnp.int32, (order, tile), 1)
            statistic = decay * picked[k, :, cols].astype(jnp.float32) + weight * product
            first[:, cols] = (jnp.where(row == col, 1.25, 0.0) - statistic * shrink).astype(
                jnp.bfloat16
            )
        new_rows[k] = stat[...] * decay + block[mine, :] * weight
        send(new_rows.at[k], new)
        if k == 0:
            for cols in columns:
                flipped[cols, :] = grad[:, cols].T
        for rest, cols, beyond in corners:
            square = dot(first[rest, :], first[:, cols], across).astype(jnp.bfloat16)
            second[rest, cols] = square
            parts = [(rest, cols)]
            if beyond.start < order:
                second[cols, beyond] = square[step:].T
                parts.append((cols, beyond))
            for here, there in parts:
                mixed[here, there] = (
                    5.0 * first[here, there].astype(jnp.float32)
                    - 4.0 * second[here, there].astype(jnp.float32)
                ).astype(jnp.bfloat16)
        for rest, cols, beyond in corners:
            power = dot(second[rest, :], second[:, cols], across).astype(jnp.bfloat16)
            fourth[rest, cols] = power
            if beyond.start < order:
                fourth[cols, beyond] = power[step:].T
        for rest, cols, beyond in corners:
            inner = dot(fourth[rest, :], mixed[:, cols], across)
            root = lift[:, :step] * (5.0 * first[rest, cols].astype(jnp.float32) - inner)
            root = root.astype(jnp.bfloat16)
            used[rest, cols] = jnp.where(due[0, k] == 1, root, picked[k, rest, cols])
            if beyond.start < order:
                flip = root[step:].T
                used[cols, beyond] = jnp.where(due[0, k] == 1, flip, picked[k, cols, beyond])
        out_rows[k] = used[mine, :]
        send(out_rows.at[k], out)

    root_of(0, left_stat, left_new, left_out)
    for cols in columns:
        x[:, cols] = dot(used[...], grad[:, cols], across).astype(jnp.bfloat16)
    root_of(1, right_stat, right_new, right_out)
    for start in range(0, order, 256):
        cols = slice(start, start + 256)
        scaled = dot(x[...], used[:, cols], across) * factor[:, :256]
        fourth[:, cols] = scaled.astype(jnp.bfloat16)
        send(fourth.at[:, cols], update.at[0, :, cols])
    for copy in sends:
        copy.wait()


def roots(total, due, place, pieces, chosen, left_stat, right_stat):
    order = chosen.shape[-1]
    tile = 512
    new = jax.ShapeDtypeStruct(left_stat.shape, jnp.float32)
    out = jax.ShapeDtypeStruct(left_stat.shape, jnp.bfloat16)
    scalar = pl.BlockSpec(memory_space=pltpu.SMEM)
    vector = pl.BlockSpec(memory_space=pltpu.VMEM)
    far = pl.BlockSpec(memory_space=pltpu.HBM)
    square = pltpu.VMEM((order, order), jnp.bfloat16)
    return pl.pallas_call(
        functools.partial(roots_kernel, tile, lax.axis_size(MP)),
        out_shape=(jax.ShapeDtypeStruct((1, order, order), jnp.bfloat16), new, new, out, out),
        in_specs=[vector, scalar, scalar, *([vector] * len(pieces)), far, vector, vector],
        out_specs=(far,) * 5,
        scratch_shapes=[
            pltpu.VMEM((2, order, order), jnp.bfloat16),
            *([square] * 8),
            pltpu.VMEM((order, order), jnp.float32),
            pltpu.VMEM((2, *left_stat.shape), jnp.float32),
            pltpu.VMEM((2, *left_stat.shape), jnp.bfloat16),
            pltpu.SemaphoreType.DMA((2,)),
            pltpu.SemaphoreType.DMA((4 + order // 256,)),
        ],
        cost_estimate=pl.CostEstimate(
            flops=10 * 2 * order**3, transcendentals=0, bytes_accessed=6 * 2**20
        ),
        compiler_params=pltpu.CompilerParams(vmem_limit_bytes=46 * 2**20),
        name="roots",
    )(total, due, place, *pieces, chosen, left_stat, right_stat)


def per_device(grad_parts, left_stat, right_stat, left_root, right_root, due):
    row_count = left_stat.shape[1]
    row_start = lax.axis_index(DP) * row_count
    chosen = choose(due, left_stat[0], right_stat[0], left_root[0], right_root[0])
    chosen, partial = lax.optimization_barrier((chosen, grad_parts[0, 0]))
    chosen = lax.all_gather(chosen, DP, axis=1, tiled=True)
    chosen = pltpu.with_memory_space_constraint(chosen, pltpu.HBM)

    part = exchange_sum(partial, WIDE)
    rows = exchange_sum(part, NARROW)
    chunk = spread(rows, ("zl", "zh"))
    side, row = lax.axis_index("zl"), lax.axis_index("y")
    middle = chunk.shape[0] // 2
    own_half = jnp.where(side == 0, chunk[:middle], chunk[middle:])
    far_half = partner(own_half, "y", 2)
    next_one = partner(chunk, "y", 1)
    last_one = partner(chunk, "y", 3)
    far_other = partner(far_half, "zl", 1)
    squares = jnp.sum(chunk.astype(jnp.float32) ** 2)
    total = jnp.full((8, 128), squares, jnp.float32)
    for axes in ("c", "x"):
        total = sum_over(total, axes)
    total = sum_over(total, "y")
    place = jnp.stack([row_start, row, side]).astype(jnp.int32)
    pieces = (chunk, next_one, last_one, far_half, far_other)
    update, left_new, right_new, left_out, right_out = roots(
        total, due, place, pieces, chosen, left_stat[0], right_stat[0]
    )
    return (update, left_new[None], right_new[None], left_out[None], right_out[None])


def solution(mesh):
    torus = Mesh(mesh.devices.reshape(4, 4, 2, 4, 2), ("y", "zh", "zl", "x", "c"))
    in_specs = (
        P(DP, MP, None, None),
        P(MP, DP, None),
        P(MP, DP, None),
        P(MP, DP, None),
        P(MP, DP, None),
        P(MP, None),
    )
    out_specs = (
        P(MP, None, None),
        P(MP, DP, None),
        P(MP, DP, None),
        P(MP, DP, None),
        P(MP, DP, None),
    )
    return jax.shard_map(
        per_device, mesh=torus, in_specs=in_specs, out_specs=out_specs, check_vma=False
    )
```

```python
import functools

import jax
import jax.numpy as jnp
from jax import lax
from jax.experimental import pallas as pl
from jax.experimental.pallas import tpu as pltpu
from jax.sharding import Mesh
from jax.sharding import PartitionSpec as P

DP = ("y", "zh", "zl")
MP = ("x", "c")
WIDE = ("y", "zl")
NARROW = "zh"

epsilon = 1e-06
decay = 0.9


def dot(a, b, dims):
    return lax.dot_general(a, b, (dims, ((), ())), preferred_element_type=jnp.float32)


def exchange_sum(value, axes):
    groups = lax.axis_size(axes)
    parts = value.reshape(groups, value.shape[0] // groups, value.shape[1])
    parts = lax.all_to_all(parts, axes, 0, 0, tiled=True)
    return jnp.sum(parts.astype(jnp.float32), 0).astype(jnp.bfloat16)


def spread(value, axes):
    groups = lax.axis_size(axes)
    copies = jnp.broadcast_to(value[None], (groups, *value.shape))
    parts = lax.all_to_all(copies, axes, 0, 0, tiled=True)
    return parts.reshape(groups * value.shape[0], value.shape[1])


def sum_over(value, axes):
    size = lax.axis_size(axes)
    parts = [value]
    for mask in range(1, size):
        swap = [(i, i ^ mask) for i in range(size)]
        parts.append(lax.ppermute(value, axes, swap))
    while len(parts) > 1:
        parts = [a + b for a, b in zip(parts[::2], parts[1::2])]
    return parts[0]


def partner(value, axis, mask):
    swap = [(i, i ^ mask) for i in range(lax.axis_size(axis))]
    return lax.ppermute(value, axis, swap)


def choose_kernel(index, due, left_stat, right_stat, left_root, right_root, chosen, *scratch):
    flags, *held, sems = scratch
    far = (due, left_stat, right_stat, left_root, right_root)
    fetches = [
        pltpu.make_async_copy(ref, near, sems.at[i])
        for i, (ref, near) in enumerate(zip(far, (flags, *held)))
    ]
    for fetch in fetches:
        fetch.start()
    for fetch in fetches:
        fetch.wait()
    for k in range(2):
        stat, root = held[k][...], held[2 + k][...]
        chosen[k] = jnp.where(flags[0, k] == 1, stat.astype(jnp.bfloat16), root)


def choose(index, *arrays):
    far = pl.BlockSpec(memory_space=pltpu.HBM)
    arrays = [pltpu.with_memory_space_constraint(a, pltpu.HBM) for a in arrays]
    due, *rows = arrays
    root = rows[-1]
    return pl.pallas_call(
        choose_kernel,
        out_shape=jax.ShapeDtypeStruct((2, *root.shape), root.dtype),
        in_specs=[pl.BlockSpec(memory_space=pltpu.SMEM), *([far] * len(arrays))],
        out_specs=pl.BlockSpec(memory_space=pltpu.VMEM),
        scratch_shapes=[
            pltpu.SMEM(due.shape, due.dtype),
            *[pltpu.VMEM(a.shape, a.dtype) for a in rows],
            pltpu.SemaphoreType.DMA((len(arrays),)),
        ],
        compiler_params=pltpu.CompilerParams(vmem_limit_bytes=4 * 2**20),
        name="choose",
    )(index, *arrays)


def halve_kernel(index, chunk, half, squares):
    rows = half.shape[0]
    side = index[0] % 2
    half[...] = chunk[pl.ds(pl.multiple_of(side * rows, rows), rows), :]
    total = jnp.zeros((32, chunk.shape[1]), jnp.float32)
    for i in range(0, chunk.shape[0], 32):
        part = chunk[i : i + 32, :].astype(jnp.float32)
        total = total + part * part
    squares[...] = jnp.full(squares.shape, jnp.sum(total), jnp.float32)


def halve(index, chunk):
    rows, order = chunk.shape
    vector = pl.BlockSpec(memory_space=pltpu.VMEM)
    return pl.pallas_call(
        halve_kernel,
        out_shape=(
            jax.ShapeDtypeStruct((rows // 2, order), chunk.dtype),
            jax.ShapeDtypeStruct((8, 128), jnp.float32),
        ),
        in_specs=[pl.BlockSpec(memory_space=pltpu.SMEM), vector],
        out_specs=(vector, vector),
        compiler_params=pltpu.CompilerParams(vmem_limit_bytes=4 * 2**20),
        name="halve",
    )(index, chunk)


def roots_kernel(tile, blocks, *refs):
    total, due, index = refs[:3]
    chunk, next_one, last_one, far_half, far_other, chosen, left_stat, right_stat = refs[3:11]
    update, left_new, right_new, left_out, right_out = refs[11:16]
    picked, grad, flipped, first, second, mixed, used, x, fourth, block = refs[16:26]
    new_rows, out_rows, sems, sent = refs[26:]
    sends = []

    def send(source, target):
        sends.append(pltpu.make_async_copy(source, target, sent.at[len(sends)]))
        sends[-1].start()

    order = chosen.shape[-1]
    rows = left_stat.shape[0]
    weight = (1.0 - decay) / order
    columns = [slice(n * tile, (n + 1) * tile) for n in range(order // tile)]
    step = 256
    corners = [
        (slice(i, order), slice(i, i + step), slice(i + step, order))
        for i in range(0, order, step)
    ]
    fetches = [
        pltpu.make_async_copy(chosen.at[k], picked.at[k], sems.at[k]) for k in range(2)
    ]
    for fetch in fetches:
        fetch.start()
    full, half = chunk.shape[0], far_half.shape[0]
    row, side = index[0] // 8, index[0] % 2
    far = (row ^ 2) * full
    for piece, at in (
        (chunk, row * full),
        (next_one, (row ^ 1) * full),
        (last_one, (row ^ 3) * full),
        (far_half, far + side * half),
        (far_other, far + (1 - side) * half),
    ):
        grad[pl.ds(pl.multiple_of(at, half), piece.shape[0]), :] = piece[...]
    mine = pl.ds(pl.multiple_of(index[0] * rows, rows), rows)
    across = ((1,), (0,))
    factor = lax.rsqrt(total[:1] / float(blocks * order * order) + epsilon)
    factor = jnp.broadcast_to(factor[:, :1], (1, tile))

    def energy():
        partial = jnp.zeros((128, order), jnp.float32)
        for i in range(0, order, 128):
            part = grad[i : i + 128, :].astype(jnp.float32)
            partial = partial + part * part
        return jnp.sum(partial)

    squares = energy()

    def scale_of(k):
        row = lax.broadcasted_iota(jnp.int32, (128, 128), 0)
        col = lax.broadcasted_iota(jnp.int32, (128, 128), 1)
        diagonal = jnp.zeros((128, 128), jnp.float32)
        for i in range(0, order, 128):
            part = picked[k, i : i + 128, i : i + 128].astype(jnp.float32)
            diagonal = diagonal + jnp.where(row == col, part, 0.0)
        return (4.0 / order) * (decay * jnp.sum(diagonal) + weight * squares)

    def root_of(k, stat, new, out):
        scale_c = jnp.zeros((1, 128), jnp.float32)
        shrink = lift = None
        for n, cols in enumerate(columns):
            if k == 0:
                product = dot(grad[...], grad[cols, :], ((1,), (1,)))
            else:
                product = dot(flipped[...], grad[:, cols], across)
            if n == 0:
                fetches[k].wait()
                scale_c = scale_c + scale_of(k)
                shrink = jnp.broadcast_to((0.25 / scale_c)[:, :1], (1, tile))
                lift = 0.25 * jnp.exp(-0.25 * jnp.log(scale_c))
                lift = jnp.broadcast_to(lift[:, :1], (1, tile))
            block[:, cols] = product
            row = lax.broadcasted_iota(jnp.int32, (order, tile), 0)
            col = n * tile + lax.broadcasted_iota(jnp.int32, (order, tile), 1)
            statistic = decay * picked[k, :, cols].astype(jnp.float32) + weight * product
            first[:, cols] = (jnp.where(row == col, 1.25, 0.0) - statistic * shrink).astype(
                jnp.bfloat16
            )
        new_rows[k] = stat[...] * decay + block[mine, :] * weight
        send(new_rows.at[k], new)
        if k == 0:
            for cols in columns:
                flipped[cols, :] = grad[:, cols].T
        for rest, cols, beyond in corners:
            square = dot(first[rest, :], first[:, cols], across).astype(jnp.bfloat16)
            second[rest, cols] = square
            parts = [(rest, cols)]
            if beyond.start < order:
                second[cols, beyond] = square[step:].T
                parts.append((cols, beyond))
            for here, there in parts:
                mixed[here, there] = (
                    5.0 * first[here, there].astype(jnp.float32)
                    - 4.0 * second[here, there].astype(jnp.float32)
                ).astype(jnp.bfloat16)
        for rest, cols, beyond in corners:
            power = dot(second[rest, :], second[:, cols], across).astype(jnp.bfloat16)
            fourth[rest, cols] = power
            if beyond.start < order:
                fourth[cols, beyond] = power[step:].T
        for rest, cols, beyond in corners:
            inner = dot(fourth[rest, :], mixed[:, cols], across)
            root = lift[:, :step] * (5.0 * first[rest, cols].astype(jnp.float32) - inner)
            root = root.astype(jnp.bfloat16)
            used[rest, cols] = jnp.where(due[0, k] == 1, root, picked[k, rest, cols])
            if beyond.start < order:
                flip = root[step:].T
                used[cols, beyond] = jnp.where(due[0, k] == 1, flip, picked[k, cols, beyond])
        out_rows[k] = used[mine, :]
        send(out_rows.at[k], out)

    root_of(0, left_stat, left_new, left_out)
    for cols in columns:
        x[:, cols] = dot(used[...], grad[:, cols], across).astype(jnp.bfloat16)
    root_of(1, right_stat, right_new, right_out)
    for start in range(0, order, 256):
        cols = slice(start, start + 256)
        scaled = dot(x[...], used[:, cols], across) * factor[:, :256]
        fourth[:, cols] = scaled.astype(jnp.bfloat16)
        send(fourth.at[:, cols], update.at[0, :, cols])
    for copy in sends:
        copy.wait()


def roots(total, due, index, pieces, chosen, left_stat, right_stat):
    order = chosen.shape[-1]
    tile = 512
    new = jax.ShapeDtypeStruct(left_stat.shape, jnp.float32)
    out = jax.ShapeDtypeStruct(left_stat.shape, jnp.bfloat16)
    scalar = pl.BlockSpec(memory_space=pltpu.SMEM)
    vector = pl.BlockSpec(memory_space=pltpu.VMEM)
    far = pl.BlockSpec(memory_space=pltpu.HBM)
    square = pltpu.VMEM((order, order), jnp.bfloat16)
    return pl.pallas_call(
        functools.partial(roots_kernel, tile, lax.axis_size(MP)),
        out_shape=(jax.ShapeDtypeStruct((1, order, order), jnp.bfloat16), new, new, out, out),
        in_specs=[vector, scalar, scalar, *([vector] * len(pieces)), far, vector, vector],
        out_specs=(far,) * 5,
        scratch_shapes=[
            pltpu.VMEM((2, order, order), jnp.bfloat16),
            *([square] * 8),
            pltpu.VMEM((order, order), jnp.float32),
            pltpu.VMEM((2, *left_stat.shape), jnp.float32),
            pltpu.VMEM((2, *left_stat.shape), jnp.bfloat16),
            pltpu.SemaphoreType.DMA((2,)),
            pltpu.SemaphoreType.DMA((4 + order // 256,)),
        ],
        cost_estimate=pl.CostEstimate(
            flops=10 * 2 * order**3, transcendentals=0, bytes_accessed=6 * 2**20
        ),
        compiler_params=pltpu.CompilerParams(vmem_limit_bytes=46 * 2**20),
        name="roots",
    )(total, due, index, *pieces, chosen, left_stat, right_stat)


def per_device(grad_parts, left_stat, right_stat, left_root, right_root, due):
    index = lax.axis_index(DP).astype(jnp.int32).reshape(1)
    chosen = choose(index, due, left_stat[0], right_stat[0], left_root[0], right_root[0])
    chosen, partial = lax.optimization_barrier((chosen, grad_parts[0, 0]))
    chosen = lax.all_gather(chosen, DP, axis=1, tiled=True)
    chosen = pltpu.with_memory_space_constraint(chosen, pltpu.HBM)

    part = exchange_sum(partial, WIDE)
    rows = exchange_sum(part, NARROW)
    chunk = spread(rows, ("zl", "zh"))
    own_half, total = halve(index, chunk)
    far_half = partner(own_half, "y", 2)
    next_one = partner(chunk, "y", 1)
    last_one = partner(chunk, "y", 3)
    total = sum_over(total, "c")
    far_other = partner(far_half, "zl", 1)
    total = sum_over(total, "x")
    total = sum_over(total, "y")
    pieces = (chunk, next_one, last_one, far_half, far_other)
    update, left_new, right_new, left_out, right_out = roots(
        total, due, index, pieces, chosen, left_stat[0], right_stat[0]
    )
    return (update, left_new[None], right_new[None], left_out[None], right_out[None])


def solution(mesh):
    torus = Mesh(mesh.devices.reshape(4, 4, 2, 4, 2), ("y", "zh", "zl", "x", "c"))
    in_specs = (
        P(DP, MP, None, None),
        P(MP, DP, None),
        P(MP, DP, None),
        P(MP, DP, None),
        P(MP, DP, None),
        P(MP, None),
    )
    out_specs = (
        P(MP, None, None),
        P(MP, DP, None),
        P(MP, DP, None),
        P(MP, DP, None),
        P(MP, DP, None),
    )
    return jax.shard_map(
        per_device, mesh=torus, in_specs=in_specs, out_specs=out_specs, check_vma=False
    )
```
